32 devices in a mesh: gx: 4 (over y, x), gy: 4 (over z), gz: 2 (over core).
Axes of the slice: x: 2, y: 2, z: 4, core: 2. Of those that a mesh axis runs over, the one named last changes fastest.
Arguments:
- positions: float32 [12, 12, 16, 96], P('gx', 'gy', 'gz'), may hold values from 0 to 1
- types: int32 [12, 12, 16, 32], P('gx', 'gy', 'gz'), may hold values from 0 to 2
Outputs:
- forces_energy: float32 [12, 12, 16, 128], P('gx', 'gy', 'gz')
The draws below stay inside these ranges and needn't reach their ends.
Inputs may be any that keep to these rules, and one draw needn't show every extreme that they name: `types`: 0 marks an empty slot, 1 a copper atom, 2 a nickel atom.
All inputs are finite; a program needn't handle non-finite values.
Results may differ from the reference program's by a relative error of at most 0.0001.
Values sent between devices are 32-bit elements; how exact they have to be, the bound alone decides.
No kernel may reach another device: no remote copies, remote signals or barrier semaphores. Data moves between devices by JAX's collectives and lax.ppermute only.
A program may use at most 64 MiB of HBM per device.

```python
import jax
import jax.numpy as jnp
from jax import lax

S = 32
NX = 12
NY = 12
NZ = 16


def set_ends(entries, key, least, top_value):
    index_at = [jax.random.randint(jax.random.fold_in(key, axis), (), 0, length) for axis, length in enumerate(entries.shape)]
    main_axis = entries.shape.index(max(entries.shape))
    beside = index_at[:main_axis] + [(index_at[main_axis] + 1) % entries.shape[main_axis]] + index_at[main_axis + 1:]
    return entries.at[tuple(index_at)].set(least).at[tuple(beside)].set(top_value)


def shard_levels(stream_key, dims, cuts, smallest, largest):
    level, own = 1.0, jax.random.fold_in(stream_key, 6)
    for axis_at, shards_of in cuts:
        draws = jnp.exp(jax.random.uniform(jax.random.fold_in(own, axis_at), (shards_of,), jnp.float32, smallest / len(cuts), largest / len(cuts)))
        level = level * jnp.repeat(draws, dims[axis_at] // shards_of).reshape([-1 if axis == axis_at else 1 for axis in range(len(dims))])
    return level


def setup_inputs(seed: int = 0) -> dict:
    key_list = jax.random.split(jax.random.key(seed), 3)
    return {
        "positions": jnp.clip(1.0 * jax.random.uniform(key_list[0], (NX, NY, NZ, 3 * S), jnp.float32) ** shard_levels(key_list[0], (NX, NY, NZ, 3 * S), ((0, 4), (1, 4), (2, 2)), -0.2, 0.2), 0.0, 1.0),
        "types": set_ends(jax.random.randint(key_list[1], (NX, NY, NZ, S), 0, 3), jax.random.fold_in(key_list[1], 1), 0, 2).astype(jnp.int32),
    }


cut_square = 0.9025
density_rate = 3.0
pair_rate = 6.0

def type_tables(types):
    weight = jnp.where(types == 1, 1.0, jnp.where(types == 2, 1.6, 0.0)).astype(jnp.float32)
    embedding = jnp.where(types == 1, 1.0, jnp.where(types == 2, 1.4, 0.0)).astype(jnp.float32)
    return (weight, embedding)

def separation(own_coords, other_coords, cell_shift):
    shift_vector = jnp.asarray(cell_shift, jnp.float32).reshape(3, 1, 1)
    displace = shift_vector + other_coords[..., :, None, :] - own_coords[..., :, :, None]
    return (displace, lax.optimization_barrier(jnp.sum(displace * displace, axis=-3)))

def density_shape(square):
    margin = jnp.maximum(1.0 - square / cut_square, 0.0)
    return jnp.exp(-density_rate * square) * margin * margin

def all_shapes(square):
    margin = jnp.maximum(1.0 - square / cut_square, 0.0)
    density_exponent = jnp.exp(-density_rate * square)
    pair_exp = jnp.exp(-pair_rate * square)
    dens_slope = -density_exponent * margin * (density_rate * margin + 2.0 / cut_square)
    pair_value = pair_exp * margin * margin
    pair_slope = -pair_exp * margin * (pair_rate * margin + 2.0 / cut_square)
    return (dens_slope, pair_value, pair_slope)

def neighbour_shifts():
    return [(a, b, c) for a in (-1, 0, 1) for b in (-1, 0, 1) for c in (-1, 0, 1)]

def reference(positions, types):
    size_x, size_y, size_z, slots = types.shape
    coords = positions.reshape(size_x, size_y, size_z, 3, slots)
    weight, embedding = type_tables(types)
    margins = ((1, 1), (1, 1), (1, 1), (0, 0))
    pad_coords = jnp.pad(coords, margins + ((0, 0),), mode='wrap')
    pad_weight = jnp.pad(weight, margins, mode='wrap')
    distinct = 1.0 - jnp.eye(slots, dtype=jnp.float32)
    plane_ids = jnp.arange(size_x).astype(jnp.int32)

    def neighbour(padded, plane_index, cell_shift):
        x_layer = lax.dynamic_index_in_dim(padded, plane_index + 1 + cell_shift[0], 0, keepdims=False)
        return x_layer[1 + cell_shift[1]:1 + cell_shift[1] + size_y, 1 + cell_shift[2]:1 + cell_shift[2] + size_z]

    def own_plane(array, plane_index):
        return lax.dynamic_index_in_dim(array, plane_index, 0, keepdims=False)

    def density_plane(plane_index):
        own_coords = own_plane(coords, plane_index)
        summed = jnp.zeros((size_y, size_z, slots), jnp.float32)
        for cell_shift in neighbour_shifts():
            other_coords = neighbour(pad_coords, plane_index, cell_shift)
            other_weight = neighbour(pad_weight, plane_index, cell_shift)
            displace, square = separation(own_coords, other_coords, cell_shift)
            dens = density_shape(square)
            if cell_shift == (0, 0, 0):
                dens = dens * distinct
            summed = summed + lax.optimization_barrier(jnp.sum(dens * other_weight[..., None, :], axis=-1))
        return summed
    density_sum = lax.map(density_plane, plane_ids)
    root_value = jnp.sqrt(density_sum + 1.0)
    slope = -embedding / (2.0 * root_value)
    pad_slope = jnp.pad(slope, margins, mode='wrap')

    def force_plane(plane_index):
        own_coords = own_plane(coords, plane_index)
        own_weight = own_plane(weight, plane_index)
        own_slope = own_plane(slope, plane_index)
        force_sum = jnp.zeros((size_y, size_z, 3, slots), jnp.float32)
        pair_sum = jnp.zeros((size_y, size_z, slots), jnp.float32)
        for cell_shift in neighbour_shifts():
            other_coords = neighbour(pad_coords, plane_index, cell_shift)
            other_weight = neighbour(pad_weight, plane_index, cell_shift)
            other_slope = neighbour(pad_slope, plane_index, cell_shift)
            displace, square = separation(own_coords, other_coords, cell_shift)
            dens_slope, pair_value, pair_slope = all_shapes(square)
            both_weight = own_weight[..., :, None] * other_weight[..., None, :]
            coupling = (own_slope[..., :, None] * other_weight[..., None, :] + other_slope[..., None, :] * own_weight[..., :, None]) * dens_slope + 0.5 * both_weight * pair_slope
            energy_pair = 0.25 * both_weight * pair_value
            if cell_shift == (0, 0, 0):
                coupling = coupling * distinct
                energy_pair = energy_pair * distinct
            force_sum = force_sum + 2.0 * lax.optimization_barrier(jnp.sum(coupling[..., None, :, :] * displace, axis=-1))
            pair_sum = pair_sum + lax.optimization_barrier(jnp.sum(energy_pair, axis=-1))
        return (force_sum, pair_sum)
    force_all, pair_all = lax.map(force_plane, plane_ids)
    energy_all = pair_all - embedding * root_value
    return jnp.concatenate([force_all.reshape(size_x, size_y, size_z, 3 * slots), energy_all], axis=-1)
```

```python
import math

import jax
import jax.numpy as jnp
from jax import lax
from jax.experimental import pallas as pl
from jax.experimental.pallas import tpu as pltpu
from jax.sharding import PartitionSpec as P

cut_square = 0.9025
density_rate = 3.0
lanes = 128

log2e = 1.0 / math.log(2.0)
unit = math.sqrt(density_rate * log2e)
reach = density_rate * log2e * cut_square
slope_offset = (2.0 / cut_square) * reach / 3.0
decay = 2.0 ** -reach
density_scale = decay / (reach * reach)
self_density = reach * reach / decay
self_energy = self_density / decay
energy_scale = 0.25 * decay * decay / (reach * reach)
force_scale = -6.0 * decay * decay / (reach * reach) / unit


def shifted(value, axis, step):
    peers = lax.axis_size(axis)
    if peers == 1:
        return value
    return lax.ppermute(value, axis, [(i, (i + step) % peers) for i in range(peers)])


def extend(value, axis, dim, width):
    length = value.shape[dim]
    last = lax.slice_in_dim(value, length - width, length, axis=dim)
    first = lax.slice_in_dim(value, 0, width, axis=dim)
    return jnp.concatenate([shifted(last, axis, 1), value, shifted(first, axis, -1)], axis=dim)


def z_peers(value):
    below = shifted(value, "gz", 1)
    above = below if lax.axis_size("gz") <= 2 else shifted(value, "gz", -1)
    return below, above


def lane_iota(rows):
    return lax.broadcasted_iota(jnp.int32, (rows, lanes), 1)


def same_cell(group):
    row = lax.broadcasted_iota(jnp.int32, (lanes, lanes), 0)
    col = lax.broadcasted_iota(jnp.int32, (lanes, lanes), 1)
    return jnp.where(row // group == col // group, 1.0, 0.0).astype(jnp.float32)


def windows(own, below, above, group):
    lane = lane_iota(own.shape[0])
    down = jnp.where(lane < group, pltpu.roll(below, group, 1), pltpu.roll(own, group, 1))
    up = jnp.where(
        lane >= lanes - group,
        pltpu.roll(above, lanes - group, 1),
        pltpu.roll(own, lanes - group, 1),
    )
    return down, own, up


def spread(rows, group, cell_sum):
    sub = lax.broadcasted_iota(jnp.int32, (group, lanes), 0)
    pick = (lane_iota(group) % group) == sub
    tall = jnp.concatenate(
        [jnp.where(pick, rows[r : r + 1], 0.0) for r in range(rows.shape[0])], axis=0
    )
    return jnp.dot(
        tall, cell_sum, precision=lax.Precision.HIGHEST, preferred_element_type=jnp.float32
    )


def gather_rows(tall, group):
    sub = lax.broadcasted_iota(jnp.int32, (group, lanes), 0)
    pick = (lane_iota(group) % group) == sub
    parts = tall.shape[0] // group
    return jnp.concatenate(
        [
            jnp.sum(jnp.where(pick, tall[p * group : (p + 1) * group], 0.0), axis=0, keepdims=True)
            for p in range(parts)
        ],
        axis=0,
    )


def fill_windows(own_ref, below_ref, above_ref, win_ref, first, size_x, size_y, parts, group):
    count = size_x * size_y

    def step(n, carry):
        x, y = n // size_y, n % size_y
        tiles = windows(
            own_ref[x + first, y + first],
            below_ref[x + first, y + first],
            above_ref[x + first, y + first],
            group,
        )
        row = lax.broadcasted_iota(jnp.int32, (4 * parts, lanes), 0)
        z_row = (row >= 2 * parts) & (row < 3 * parts)
        for k, tile in enumerate(tiles):
            win_ref[n * 3 + k] = tile + jnp.where(z_row, (k - 1) * unit, 0.0) if k != 1 else tile
        return carry

    lax.fori_loop(0, count, step, 0)


def density_kernel(own_ref, below_ref, above_ref, rows_ref, full_ref, win_ref, *, slots, group):
    wide_x, wide_y = own_ref.shape[0], own_ref.shape[1]
    parts = slots // group
    cell_sum = same_cell(group)
    fill_windows(own_ref, below_ref, above_ref, win_ref, 0, wide_x, wide_y, parts, group)
    inner_x, inner_y = wide_x - 2, wide_y - 2

    def column(n, carry):
        x, y = n // inner_y, n % inner_y
        rows = own_ref[x + 1, y + 1]
        own = spread(rows, group, cell_sum)
        px, py, pz, pw = [own[c * slots : (c + 1) * slots] for c in range(4)]

        def side(o, total):
            dx, dy = o // 3, o % 3
            base = ((x + dx) * wide_y + (y + dy)) * 3
            sx = (dx - 1).astype(jnp.float32) * unit
            sy = (dy - 1).astype(jnp.float32) * unit
            for k in range(3):
                tile = win_ref[base + k]
                for p in range(parts):
                    jx, jy, jz, jw = [tile[c * parts + p : c * parts + p + 1] for c in range(4)]
                    ax, ay, az = (jx + sx) - px, (jy + sy) - py, jz - pz
                    margin = jnp.maximum(reach - (ax * ax + ay * ay + az * az), 0.0)
                    total = total + (jnp.exp2(margin) * margin) * (margin * jw)
            return total

        total = lax.fori_loop(0, 9, side, jnp.zeros((slots, lanes), jnp.float32))
        total = jnp.dot(
            total, cell_sum, precision=lax.Precision.HIGHEST, preferred_element_type=jnp.float32
        )
        root = jnp.sqrt((total - self_density * pw) * density_scale + 1.0)
        full_ref[n] = root
        ratio = jnp.where(pw > 1.2, 1.4 / 1.6, jnp.where(pw > 0.0, 1.0, 0.0))
        rows_ref[n] = gather_rows(-ratio * (0.5 / decay) / root, group)
        return carry

    lax.fori_loop(0, inner_x * inner_y, column, 0)


def force_kernel(
    own_ref, below_ref, above_ref, root_ref, slope_ref, slope_below_ref, slope_above_ref,
    out_ref, win_ref, slope_win_ref, *, slots, group
):
    size_x, size_y, cells_z = out_ref.shape[0], out_ref.shape[1], out_ref.shape[2]
    wide_y = size_y + 2
    parts = slots // group
    cell_sum = same_cell(group)
    fill_windows(own_ref, below_ref, above_ref, win_ref, 1, size_x + 2, wide_y, parts, group)

    def slope_step(n, carry):
        tiles = windows(slope_ref[n], slope_below_ref[n], slope_above_ref[n], group)
        for k, tile in enumerate(tiles):
            slope_win_ref[n * 3 + k] = tile
        return carry

    lax.fori_loop(0, (size_x + 2) * wide_y, slope_step, 0)
    of_cell = jnp.where(
        lax.broadcasted_iota(jnp.int32, (cells_z, lanes), 1) // group
        == lax.broadcasted_iota(jnp.int32, (cells_z, lanes), 0),
        1.0,
        0.0,
    ).astype(jnp.float32)

    def column(n, carry):
        x, y = n // size_y, n % size_y
        here = (x + 1) * wide_y + y + 1
        own = spread(own_ref[x + 2, y + 2], group, cell_sum)
        px, py, pz, pw = [own[c * slots : (c + 1) * slots] for c in range(4)]
        root = root_ref[here]
        pt = -jnp.where(pw > 1.2, 1.4 / 1.6, jnp.where(pw > 0.0, 1.0, 0.0)) * (0.5 / decay) / root

        def side(o, sums):
            fx, fy, fz, en = sums
            dx, dy = o // 3, o % 3
            base = ((x + dx) * wide_y + (y + dy)) * 3
            sx = (dx - 1).astype(jnp.float32) * unit
            sy = (dy - 1).astype(jnp.float32) * unit
            for k in range(3):
                tile = win_ref[base + k]
                slope_tile = slope_win_ref[base + k]
                for p in range(parts):
                    jx, jy, jz, jw = [tile[c * parts + p : c * parts + p + 1] for c in range(4)]
                    jt = slope_tile[p : p + 1]
                    ax, ay, az = (jx + sx) - px, (jy + sy) - py, jz - pz
                    margin = jnp.maximum(reach - (ax * ax + ay * ay + az * az), 0.0)
                    power = jnp.exp2(margin)
                    edge = power * margin
                    weighted = edge * jw
                    v = weighted * (
                        (pt + jt) * (margin + slope_offset) + power * (margin + 0.5 * slope_offset)
                    )
                    fx, fy, fz = fx + v * ax, fy + v * ay, fz + v * az
                    en = en + weighted * edge
            return fx, fy, fz, en

        zero = jnp.zeros((slots, lanes), jnp.float32)
        fx, fy, fz, en = lax.fori_loop(0, 9, side, (zero, zero, zero, zero))
        embedding = jnp.where(pw > 1.2, 1.4, pw)
        scale = force_scale * pw
        energy = (en - (self_energy / group) * pw) * (energy_scale * pw) - embedding * root / group
        tall = jnp.concatenate([fx * scale, fy * scale, fz * scale, energy], axis=0)
        out_ref[x, y] = lax.dot_general(
            of_cell, tall, (((1,), (1,)), ((), ())),
            precision=lax.Precision.HIGHEST, preferred_element_type=jnp.float32,
        )
        return carry

    lax.fori_loop(0, size_x * size_y, column, 0)


def body(positions, types):
    size_x, size_y, cells_z, slots = types.shape
    group = lanes // cells_z
    parts = slots // group
    weight = jnp.where(types == 1, 1.0, jnp.where(types == 2, 1.6, 0.0)).astype(jnp.float32)
    value = jnp.concatenate([positions * unit, weight], axis=3)
    value = value.reshape(size_x, size_y, cells_z, 4 * parts, group)
    value = value.transpose(0, 1, 3, 2, 4).reshape(size_x, size_y, 4 * parts, lanes)
    value = extend(extend(value, "gx", 0, 2), "gy", 1, 2)
    below, above = z_peers(value)
    columns = (size_x + 2) * (size_y + 2)
    f32 = jnp.float32
    slope_rows, root = pl.pallas_call(
        lambda *refs: density_kernel(*refs, slots=slots, group=group),
        out_shape=(
            jax.ShapeDtypeStruct((columns, parts, lanes), f32),
            jax.ShapeDtypeStruct((columns, slots, lanes), f32),
        ),
        scratch_shapes=[
            pltpu.VMEM(((size_x + 4) * (size_y + 4) * 3, 4 * parts, lanes), f32)
        ],
        name="density",
    )(value, below, above)
    slope_below, slope_above = z_peers(slope_rows)
    return pl.pallas_call(
        lambda *refs: force_kernel(*refs, slots=slots, group=group),
        out_shape=jax.ShapeDtypeStruct((size_x, size_y, cells_z, 4 * slots), f32),
        scratch_shapes=[
            pltpu.VMEM((columns * 3, 4 * parts, lanes), f32),
            pltpu.VMEM((columns * 3, parts, lanes), f32),
        ],
        name="force",
    )(value, below, above, root, slope_rows, slope_below, slope_above)


def solution(mesh):
    in_specs = (P("gx", "gy", "gz", None), P("gx", "gy", "gz", None))
    out_specs = P("gx", "gy", "gz", None)
    return jax.shard_map(body, mesh=mesh, in_specs=in_specs, out_specs=out_specs, check_vma=False)
```

```python
import math

import jax
import jax.numpy as jnp
from jax import lax
from jax.experimental import pallas as pl
from jax.experimental.pallas import tpu as pltpu
from jax.sharding import PartitionSpec as P

cut_square = 0.9025
density_rate = 3.0
lanes = 128

log2e = 1.0 / math.log(2.0)
unit = math.sqrt(density_rate * log2e)
reach = density_rate * log2e * cut_square
slope_offset = (2.0 / cut_square) * reach / 3.0
decay = 2.0 ** -reach
density_scale = decay / (reach * reach)
self_density = reach * reach / decay
self_energy = self_density / decay
energy_scale = 0.25 * decay * decay / (reach * reach)
force_scale = -6.0 * decay * decay / (reach * reach) / unit


def shifted(value, axis, step):
    peers = lax.axis_size(axis)
    if peers == 1:
        return value
    return lax.ppermute(value, axis, [(i, (i + step) % peers) for i in range(peers)])


def extend(value, axis, dim, width):
    length = value.shape[dim]
    last = lax.slice_in_dim(value, length - width, length, axis=dim)
    first = lax.slice_in_dim(value, 0, width, axis=dim)
    return jnp.concatenate([shifted(last, axis, 1), value, shifted(first, axis, -1)], axis=dim)


def z_peers(value):
    below = shifted(value, "gz", 1)
    above = below if lax.axis_size("gz") <= 2 else shifted(value, "gz", -1)
    return below, above


def lane_iota(rows):
    return lax.broadcasted_iota(jnp.int32, (rows, lanes), 1)


def same_cell(group):
    row = lax.broadcasted_iota(jnp.int32, (lanes, lanes), 0)
    col = lax.broadcasted_iota(jnp.int32, (lanes, lanes), 1)
    return jnp.where(row // group == col // group, 1.0, 0.0).astype(jnp.float32)


def windows(own, below, above, group):
    lane = lane_iota(own.shape[0])
    down = jnp.where(lane < group, pltpu.roll(below, group, 1), pltpu.roll(own, group, 1))
    up = jnp.where(
        lane >= lanes - group,
        pltpu.roll(above, lanes - group, 1),
        pltpu.roll(own, lanes - group, 1),
    )
    return down, own, up


def pieces(value):
    parts = []
    for _ in range(3):
        part = value.astype(jnp.bfloat16)
        parts.append(part)
        value = value - part.astype(jnp.float32)
    return parts


def exact_dot(value, ones, contract):
    ones = ones.astype(jnp.bfloat16)
    total = None
    for part in pieces(value):
        left, right = (ones, part) if contract == 1 else (part, ones)
        term = lax.dot_general(
            left, right, (((1,), (contract,)), ((), ())), preferred_element_type=jnp.float32
        )
        total = term if total is None else total + term
    return total


def pick_mask(group):
    sub = lax.broadcasted_iota(jnp.int32, (group, lanes), 0)
    return (lane_iota(group) % group) == sub


def spread(rows, group, cell_sum):
    pick = pick_mask(group)
    total = None
    ones = cell_sum.astype(jnp.bfloat16)
    for part in pieces(rows):
        part = part.astype(jnp.float32)
        tall = jnp.concatenate(
            [jnp.where(pick, part[r : r + 1], 0.0) for r in range(rows.shape[0])], axis=0
        ).astype(jnp.bfloat16)
        term = jnp.dot(tall, ones, preferred_element_type=jnp.float32)
        total = term if total is None else total + term
    return total


def gather_rows(tall, group):
    pick = pick_mask(group)
    parts = tall.shape[0] // group
    return jnp.concatenate(
        [
            jnp.sum(jnp.where(pick, tall[p * group : (p + 1) * group], 0.0), axis=0, keepdims=True)
            for p in range(parts)
        ],
        axis=0,
    )


def placed(rows, x, y, parts):
    row = lax.broadcasted_iota(jnp.int32, rows.shape, 0)
    along_x = jnp.where(row < parts, unit, 0.0)
    along_y = jnp.where((row >= parts) & (row < 2 * parts), unit, 0.0)
    at_x, at_y = jnp.asarray(x).astype(jnp.float32), jnp.asarray(y).astype(jnp.float32)
    return rows + (along_x * at_x + along_y * at_y)


def fill_windows(own_ref, below_ref, above_ref, win_ref, square_ref, first, count_x, count_y,
                 parts, group):
    center_x = 0.5 * (count_x - 1)
    center_y = 0.5 * (count_y - 1)
    row = lax.broadcasted_iota(jnp.int32, (4 * parts, lanes), 0)
    z_step = jnp.where((row >= 2 * parts) & (row < 3 * parts), unit, 0.0)

    def step(x, carry):
        for y in range(count_y):
            tiles = windows(
                own_ref[x + first, y + first],
                below_ref[x + first, y + first],
                above_ref[x + first, y + first],
                group,
            )
            for k, tile in enumerate(tiles):
                tile = placed(tile, x - center_x, y - center_y, parts) + (k - 1.0) * z_step
                n = (x * count_y + y) * 3 + k
                win_ref[n] = tile
                if square_ref is not None:
                    square = tile * tile
                    square_ref[n] = -(
                        square[:parts] + square[parts : 2 * parts] + square[2 * parts : 3 * parts]
                    )
        return carry

    lax.fori_loop(0, count_x, step, 0)


def type_ratio(weight):
    return jnp.where(weight > 1.2, 1.4 / 1.6, jnp.where(weight > 0.0, 1.0, 0.0))


def density_kernel(own_ref, below_ref, above_ref, rows_ref, root_ref, win_ref, square_ref,
                   full_ref, sum_ref, *, slots, group):
    wide_x, wide_y = own_ref.shape[0], own_ref.shape[1]
    parts = slots // group
    cell_sum = same_cell(group)
    fill_windows(own_ref, below_ref, above_ref, win_ref, square_ref, 0, wide_x, wide_y, parts,
                 group)
    inner_x, inner_y = wide_x - 2, wide_y - 2

    def spread_step(x, carry):
        for y in range(inner_y):
            rows = win_ref[((x + 1) * wide_y + y + 1) * 3 + 1]
            full_ref[x * inner_y + y] = spread(rows, group, cell_sum)
        return carry

    lax.fori_loop(0, inner_x, spread_step, 0)

    def column(n, carry):
        x, y = n // inner_y, n % inner_y
        px, py, pz = [full_ref[n, c * slots : (c + 1) * slots, :] for c in range(3)]
        room = reach - (px * px + py * py + pz * pz)
        px, py, pz = px + px, py + py, pz + pz

        def side(dx, total):
            base = ((x + dx) * wide_y + y) * 3
            for m in range(9):
                for p in range(parts):
                    jx, jy, jz, jw = [
                        win_ref[base + m, c * parts + p : c * parts + p + 1, :] for c in range(4)
                    ]
                    js = square_ref[base + m, p : p + 1, :]
                    margin = jnp.maximum((room + js) + px * jx + (py * jy + pz * jz), 0.0)
                    total = total + (jnp.exp2(margin) * margin) * (margin * jw)
            return total

        sum_ref[n] = lax.fori_loop(0, 3, side, jnp.zeros((slots, lanes), jnp.float32))
        return carry

    lax.fori_loop(0, inner_x * inner_y, column, 0)

    def finish(x, carry):
        for y in range(inner_y):
            n = x * inner_y + y
            pw = full_ref[n, 3 * slots : 4 * slots, :]
            total = exact_dot(sum_ref[n], cell_sum, 0)
            density = jnp.maximum(total - self_density * pw, 0.0) * density_scale
            root = jnp.sqrt(density + 1.0)
            root_ref[n] = root
            rows_ref[n] = gather_rows(-type_ratio(pw) * (0.5 / decay) / root, group)
        return carry

    lax.fori_loop(0, inner_x, finish, 0)


def force_kernel(
    own_ref, below_ref, above_ref, root_ref, slope_ref, slope_below_ref, slope_above_ref,
    out_ref, win_ref, slope_win_ref, full_ref, sum_ref, *, slots, group
):
    size_x, size_y, cells_z = out_ref.shape[0], out_ref.shape[1], out_ref.shape[2]
    wide_x, wide_y = size_x + 2, size_y + 2
    parts = slots // group
    cell_sum = same_cell(group)
    fill_windows(own_ref, below_ref, above_ref, win_ref, None, 1, wide_x, wide_y, parts, group)

    def slope_step(x, carry):
        for y in range(wide_y):
            n = x * wide_y + y
            tiles = windows(slope_ref[n], slope_below_ref[n], slope_above_ref[n], group)
            for k, tile in enumerate(tiles):
                slope_win_ref[n * 3 + k] = tile
        return carry

    lax.fori_loop(0, wide_x, slope_step, 0)
    of_cell = jnp.where(
        lane_iota(cells_z) // group == lax.broadcasted_iota(jnp.int32, (cells_z, lanes), 0),
        1.0,
        0.0,
    ).astype(jnp.float32)

    def spread_step(x, carry):
        for y in range(size_y):
            rows = win_ref[((x + 1) * wide_y + y + 1) * 3 + 1]
            full_ref[x * size_y + y] = spread(rows, group, cell_sum)
        return carry

    lax.fori_loop(0, size_x, spread_step, 0)
    half = slots // 2

    def column(n, carry):
        x, y = n // size_y, n % size_y
        here = (x + 1) * wide_y + y + 1
        for start in (0, half):
            px, py, pz, pw = [
                full_ref[n, c * slots + start : c * slots + start + half, :] for c in range(4)
            ]
            root = root_ref[here, start : start + half, :]
            pt = -type_ratio(pw) * (0.5 / decay) / root

            def side(dx, sums):
                fx, fy, fz, en = sums
                base = ((x + dx) * wide_y + y) * 3
                for m in range(9):
                    for p in range(parts):
                        jx, jy, jz, jw = [
                            win_ref[base + m, c * parts + p : c * parts + p + 1, :]
                            for c in range(4)
                        ]
                        jt = slope_win_ref[base + m, p : p + 1, :]
                        ax, ay, az = jx - px, jy - py, jz - pz
                        margin = jnp.maximum(reach - (ax * ax + ay * ay + az * az), 0.0)
                        power = jnp.exp2(margin)
                        edge = power * margin
                        weighted = edge * jw
                        v = weighted * (
                            (pt + jt) * (margin + slope_offset)
                            + power * (margin + 0.5 * slope_offset)
                        )
                        fx, fy, fz = fx + v * ax, fy + v * ay, fz + v * az
                        en = en + weighted * edge
                return fx, fy, fz, en

            zero = jnp.zeros((half, lanes), jnp.float32)
            fx, fy, fz, en = lax.fori_loop(0, 3, side, (zero, zero, zero, zero))
            embedding = jnp.where(pw > 1.2, 1.4, pw)
            scale = force_scale * pw
            sum_ref[n, start : start + half, :] = fx * scale
            sum_ref[n, slots + start : slots + start + half, :] = fy * scale
            sum_ref[n, 2 * slots + start : 2 * slots + start + half, :] = fz * scale
            sum_ref[n, 3 * slots + start : 3 * slots + start + half, :] = (
                en - (self_energy / group) * pw
            ) * (energy_scale * pw) - embedding * root * (1.0 / group)
        return carry

    lax.fori_loop(0, size_x * size_y, column, 0)

    def finish(x, carry):
        for y in range(size_y):
            out_ref[x, y] = exact_dot(sum_ref[x * size_y + y], of_cell, 1)
        return carry

    lax.fori_loop(0, size_x, finish, 0)


def body(positions, types):
    size_x, size_y, cells_z, slots = types.shape
    group = lanes // cells_z
    parts = slots // group
    weight = jnp.where(types == 1, 1.0, jnp.where(types == 2, 1.6, 0.0)).astype(jnp.float32)
    value = jnp.concatenate([positions * unit, weight], axis=3)
    value = value.reshape(size_x, size_y, cells_z, 4 * parts, group)
    value = value.transpose(0, 1, 3, 2, 4).reshape(size_x, size_y, 4 * parts, lanes)
    value = extend(extend(value, "gx", 0, 2), "gy", 1, 2)
    below, above = z_peers(value)
    columns = (size_x + 2) * (size_y + 2)
    f32 = jnp.float32
    slope_rows, root = pl.pallas_call(
        lambda *refs: density_kernel(*refs, slots=slots, group=group),
        out_shape=(
            jax.ShapeDtypeStruct((columns, parts, lanes), f32),
            jax.ShapeDtypeStruct((columns, slots, lanes), f32),
        ),
        scratch_shapes=[
            pltpu.VMEM(((size_x + 4) * (size_y + 4) * 3, 4 * parts, lanes), f32),
            pltpu.VMEM(((size_x + 4) * (size_y + 4) * 3, parts, lanes), f32),
            pltpu.VMEM((columns, 4 * slots, lanes), f32),
            pltpu.VMEM((columns, slots, lanes), f32),
        ],
        name="density",
    )(value, below, above)
    slope_below, slope_above = z_peers(slope_rows)
    return pl.pallas_call(
        lambda *refs: force_kernel(*refs, slots=slots, group=group),
        out_shape=jax.ShapeDtypeStruct((size_x, size_y, cells_z, 4 * slots), f32),
        scratch_shapes=[
            pltpu.VMEM((columns * 3, 4 * parts, lanes), f32),
            pltpu.VMEM((columns * 3, parts, lanes), f32),
            pltpu.VMEM((size_x * size_y, 4 * slots, lanes), f32),
            pltpu.VMEM((size_x * size_y, 4 * slots, lanes), f32),
        ],
        name="force",
    )(value, below, above, root, slope_rows, slope_below, slope_above)


def solution(mesh):
    in_specs = (P("gx", "gy", "gz", None), P("gx", "gy", "gz", None))
    out_specs = P("gx", "gy", "gz", None)
    return jax.shard_map(body, mesh=mesh, in_specs=in_specs, out_specs=out_specs, check_vma=False)
```

```python
import math

import jax
import jax.numpy as jnp
from jax import lax
from jax.experimental import pallas as pl
from jax.experimental.pallas import tpu as pltpu
from jax.sharding import PartitionSpec as P

cut_square = 0.9025
density_rate = 3.0
lanes = 128

log2e = 1.0 / math.log(2.0)
unit = math.sqrt(density_rate * log2e)
reach = density_rate * log2e * cut_square
slope_offset = (2.0 / cut_square) * reach / 3.0
decay = 2.0 ** -reach
density_scale = decay / (reach * reach)
self_density = reach * reach / decay
self_energy = self_density / decay
energy_scale = 0.25 * decay * decay / (reach * reach)
force_scale = -6.0 * decay * decay / (reach * reach) / unit


def shifted(value, axis, step):
    peers = lax.axis_size(axis)
    if peers == 1:
        return value
    return lax.ppermute(value, axis, [(i, (i + step) % peers) for i in range(peers)])


def extend(value, axis, dim, width):
    length = value.shape[dim]
    last = lax.slice_in_dim(value, length - width, length, axis=dim)
    first = lax.slice_in_dim(value, 0, width, axis=dim)
    return jnp.concatenate([shifted(last, axis, 1), value, shifted(first, axis, -1)], axis=dim)


def z_peers(value):
    below = shifted(value, "gz", 1)
    above = below if lax.axis_size("gz") <= 2 else shifted(value, "gz", -1)
    return below, above


def lane_iota(rows):
    return lax.broadcasted_iota(jnp.int32, (rows, lanes), 1)


def same_cell(group):
    row = lax.broadcasted_iota(jnp.int32, (lanes, lanes), 0)
    col = lax.broadcasted_iota(jnp.int32, (lanes, lanes), 1)
    return jnp.where(row // group == col // group, 1.0, 0.0).astype(jnp.float32)


def windows(own, below, above, group):
    lane = lane_iota(own.shape[0])
    down = jnp.where(lane < group, pltpu.roll(below, group, 1), pltpu.roll(own, group, 1))
    up = jnp.where(
        lane >= lanes - group,
        pltpu.roll(above, lanes - group, 1),
        pltpu.roll(own, lanes - group, 1),
    )
    return down, own, up


def pieces(value):
    parts = []
    for _ in range(3):
        part = value.astype(jnp.bfloat16)
        parts.append(part)
        value = value - part.astype(jnp.float32)
    return parts


def exact_dot(value, ones, contract):
    ones = ones.astype(jnp.bfloat16)
    total = None
    for part in pieces(value):
        left, right = (ones, part) if contract == 1 else (part, ones)
        term = lax.dot_general(
            left, right, (((1,), (contract,)), ((), ())), preferred_element_type=jnp.float32
        )
        total = term if total is None else total + term
    return total


def pick_mask(group):
    sub = lax.broadcasted_iota(jnp.int32, (group, lanes), 0)
    return (lane_iota(group) % group) == sub


def spread(rows, group, cell_sum):
    pick = pick_mask(group)
    total = None
    ones = cell_sum.astype(jnp.bfloat16)
    for part in pieces(rows):
        part = part.astype(jnp.float32)
        tall = jnp.concatenate(
            [jnp.where(pick, part[r : r + 1], 0.0) for r in range(rows.shape[0])], axis=0
        ).astype(jnp.bfloat16)
        term = jnp.dot(tall, ones, preferred_element_type=jnp.float32)
        total = term if total is None else total + term
    return total


def gather_rows(tall, group):
    pick = pick_mask(group)
    parts = tall.shape[0] // group
    return jnp.concatenate(
        [
            jnp.sum(jnp.where(pick, tall[p * group : (p + 1) * group], 0.0), axis=0, keepdims=True)
            for p in range(parts)
        ],
        axis=0,
    )


def placed(rows, x, y, parts):
    row = lax.broadcasted_iota(jnp.int32, rows.shape, 0)
    along_x = jnp.where(row < parts, unit, 0.0)
    along_y = jnp.where((row >= parts) & (row < 2 * parts), unit, 0.0)
    at_x, at_y = jnp.asarray(x).astype(jnp.float32), jnp.asarray(y).astype(jnp.float32)
    return rows + (along_x * at_x + along_y * at_y)


def fill_windows(own_ref, below_ref, above_ref, win_ref, square_ref, first, count_x, count_y,
                 parts, group):
    center_x = 0.5 * (count_x - 1)
    center_y = 0.5 * (count_y - 1)
    row = lax.broadcasted_iota(jnp.int32, (4 * parts, lanes), 0)
    z_step = jnp.where((row >= 2 * parts) & (row < 3 * parts), unit, 0.0)

    def step(x, carry):
        for y in range(count_y):
            tiles = windows(
                own_ref[x + first, y + first],
                below_ref[x + first, y + first],
                above_ref[x + first, y + first],
                group,
            )
            for k, tile in enumerate(tiles):
                tile = placed(tile, x - center_x, y - center_y, parts) + (k - 1.0) * z_step
                n = (x * count_y + y) * 3 + k
                win_ref[n] = tile
                if square_ref is not None:
                    square = tile * tile
                    square_ref[n] = -(
                        square[:parts] + square[parts : 2 * parts] + square[2 * parts : 3 * parts]
                    )
        return carry

    lax.fori_loop(0, count_x, step, 0)


def type_ratio(weight):
    return jnp.where(weight > 1.2, 1.4 / 1.6, jnp.where(weight > 0.0, 1.0, 0.0))


def density_kernel(own_ref, below_ref, above_ref, rows_ref, win_ref, square_ref, full_ref,
                   sum_ref, *, slots, group):
    wide_x, wide_y = own_ref.shape[0], own_ref.shape[1]
    parts = slots // group
    cell_sum = same_cell(group)
    fill_windows(own_ref, below_ref, above_ref, win_ref, square_ref, 0, wide_x, wide_y, parts,
                 group)
    inner_x, inner_y = wide_x - 2, wide_y - 2

    def spread_step(x, carry):
        for y in range(inner_y):
            rows = win_ref[((x + 1) * wide_y + y + 1) * 3 + 1]
            full_ref[x * inner_y + y] = spread(rows, group, cell_sum)
        return carry

    lax.fori_loop(0, inner_x, spread_step, 0)

    def column(n, carry):
        x, y = n // inner_y, n % inner_y
        px, py, pz = [full_ref[n, c * slots : (c + 1) * slots, :] for c in range(3)]
        room = reach - (px * px + py * py + pz * pz)
        px, py, pz = px + px, py + py, pz + pz

        total = jnp.zeros((slots, lanes), jnp.float32)
        for dx in range(3):
            base = ((x + dx) * wide_y + y) * 3
            for m in range(9):
                for p in range(parts):
                    jx, jy, jz, jw = [
                        win_ref[base + m, c * parts + p : c * parts + p + 1, :] for c in range(4)
                    ]
                    js = square_ref[base + m, p : p + 1, :]
                    margin = jnp.maximum((room + js) + px * jx + (py * jy + pz * jz), 0.0)
                    total = total + (jnp.exp2(margin) * margin) * (margin * jw)
        sum_ref[n] = total
        return carry

    lax.fori_loop(0, inner_x * inner_y, column, 0)

    def finish(x, carry):
        for y in range(inner_y):
            n = x * inner_y + y
            pw = full_ref[n, 3 * slots : 4 * slots, :]
            total = exact_dot(sum_ref[n], cell_sum, 0)
            density = jnp.maximum(total - self_density * pw, 0.0) * density_scale
            rows_ref[n] = gather_rows(jnp.sqrt(density + 1.0), group)
        return carry

    lax.fori_loop(0, inner_x, finish, 0)


def force_kernel(
    own_ref, below_ref, above_ref, rows_ref, rows_below_ref, rows_above_ref,
    out_ref, win_ref, slope_win_ref, full_ref, sum_ref, *, slots, group
):
    size_x, size_y, cells_z = out_ref.shape[0], out_ref.shape[1], out_ref.shape[2]
    wide_x, wide_y = size_x + 2, size_y + 2
    parts = slots // group
    cell_sum = same_cell(group)
    fill_windows(own_ref, below_ref, above_ref, win_ref, None, 1, wide_x, wide_y, parts, group)

    def slope_step(x, carry):
        for y in range(wide_y):
            n = x * wide_y + y
            tiles = windows(rows_ref[n], rows_below_ref[n], rows_above_ref[n], group)
            for k, tile in enumerate(tiles):
                weight = win_ref[n * 3 + k, 3 * parts : 4 * parts, :]
                slope_win_ref[n * 3 + k] = -type_ratio(weight) * (0.5 / decay) / tile
        return carry

    lax.fori_loop(0, wide_x, slope_step, 0)
    of_cell = jnp.where(
        lane_iota(cells_z) // group == lax.broadcasted_iota(jnp.int32, (cells_z, lanes), 0),
        1.0,
        0.0,
    ).astype(jnp.float32)

    def spread_step(x, carry):
        for y in range(size_y):
            rows = win_ref[((x + 1) * wide_y + y + 1) * 3 + 1]
            rows = jnp.concatenate([rows, rows_ref[(x + 1) * wide_y + y + 1]], axis=0)
            full_ref[x * size_y + y] = spread(rows, group, cell_sum)
        return carry

    lax.fori_loop(0, size_x, spread_step, 0)
    half = slots // 2

    def column(n, carry):
        x, y = n // size_y, n % size_y
        for start in (0, half):
            px, py, pz, pw, root = [
                full_ref[n, c * slots + start : c * slots + start + half, :] for c in range(5)
            ]
            pt = -type_ratio(pw) * (0.5 / decay) / root

            def side(dx, sums):
                fx, fy, fz, en = sums
                base = ((x + dx) * wide_y + y) * 3
                for m in range(9):
                    for p in range(parts):
                        jx, jy, jz, jw = [
                            win_ref[base + m, c * parts + p : c * parts + p + 1, :]
                            for c in range(4)
                        ]
                        jt = slope_win_ref[base + m, p : p + 1, :]
                        ax, ay, az = jx - px, jy - py, jz - pz
                        margin = jnp.maximum(reach - (ax * ax + ay * ay + az * az), 0.0)
                        power = jnp.exp2(margin)
                        edge = power * margin
                        weighted = edge * jw
                        v = weighted * (
                            (pt + jt) * (margin + slope_offset)
                            + power * (margin + 0.5 * slope_offset)
                        )
                        fx, fy, fz = fx + v * ax, fy + v * ay, fz + v * az
                        en = en + weighted * edge
                return fx, fy, fz, en

            zero = jnp.zeros((half, lanes), jnp.float32)
            fx, fy, fz, en = lax.fori_loop(0, 3, side, (zero, zero, zero, zero))
            embedding = jnp.where(pw > 1.2, 1.4, pw)
            scale = force_scale * pw
            sum_ref[n, start : start + half, :] = fx * scale
            sum_ref[n, slots + start : slots + start + half, :] = fy * scale
            sum_ref[n, 2 * slots + start : 2 * slots + start + half, :] = fz * scale
            sum_ref[n, 3 * slots + start : 3 * slots + start + half, :] = (
                en - (self_energy / group) * pw
            ) * (energy_scale * pw) - embedding * root * (1.0 / group)
        return carry

    lax.fori_loop(0, size_x * size_y, column, 0)

    def finish(x, carry):
        for y in range(size_y):
            out_ref[x, y] = exact_dot(sum_ref[x * size_y + y], of_cell, 1)
        return carry

    lax.fori_loop(0, size_x, finish, 0)


def body(positions, types):
    size_x, size_y, cells_z, slots = types.shape
    group = lanes // cells_z
    parts = slots // group
    weight = jnp.where(types == 1, 1.0, jnp.where(types == 2, 1.6, 0.0)).astype(jnp.float32)
    value = jnp.concatenate([positions * unit, weight], axis=3)
    value = value.reshape(size_x, size_y, cells_z, 4 * parts, group)
    value = value.transpose(0, 1, 3, 2, 4).reshape(size_x, size_y, 4 * parts, lanes)
    value = extend(extend(value, "gx", 0, 2), "gy", 1, 2)
    below, above = z_peers(value)
    columns = (size_x + 2) * (size_y + 2)
    f32 = jnp.float32
    root_rows = pl.pallas_call(
        lambda *refs: density_kernel(*refs, slots=slots, group=group),
        out_shape=jax.ShapeDtypeStruct((columns, parts, lanes), f32),
        scratch_shapes=[
            pltpu.VMEM(((size_x + 4) * (size_y + 4) * 3, 4 * parts, lanes), f32),
            pltpu.VMEM(((size_x + 4) * (size_y + 4) * 3, parts, lanes), f32),
            pltpu.VMEM((columns, 4 * slots, lanes), f32),
            pltpu.VMEM((columns, slots, lanes), f32),
        ],
        name="density",
    )(value, below, above)
    root_below, root_above = z_peers(root_rows)
    return pl.pallas_call(
        lambda *refs: force_kernel(*refs, slots=slots, group=group),
        out_shape=jax.ShapeDtypeStruct((size_x, size_y, cells_z, 4 * slots), f32),
        scratch_shapes=[
            pltpu.VMEM((columns * 3, 4 * parts, lanes), f32),
            pltpu.VMEM((columns * 3, parts, lanes), f32),
            pltpu.VMEM((size_x * size_y, 5 * slots, lanes), f32),
            pltpu.VMEM((size_x * size_y, 4 * slots, lanes), f32),
        ],
        name="force",
    )(value, below, above, root_rows, root_below, root_above)


def solution(mesh):
    in_specs = (P("gx", "gy", "gz", None), P("gx", "gy", "gz", None))
    out_specs = P("gx", "gy", "gz", None)
    return jax.shard_map(body, mesh=mesh, in_specs=in_specs, out_specs=out_specs, check_vma=False)
```

```python
import math

import jax
import jax.numpy as jnp
from jax import lax
from jax.experimental import pallas as pl
from jax.experimental.pallas import tpu as pltpu
from jax.sharding import PartitionSpec as P

cut_square = 0.9025
density_rate = 3.0
lanes = 128

log2e = 1.0 / math.log(2.0)
unit = math.sqrt(density_rate * log2e)
reach = density_rate * log2e * cut_square
slope_offset = (2.0 / cut_square) * reach / 3.0
decay = 2.0 ** -reach
density_scale = decay / (reach * reach)
self_density = reach * reach / decay
self_energy = self_density / decay
energy_scale = 0.25 * decay * decay / (reach * reach)
force_scale = -6.0 * decay * decay / (reach * reach) / unit


def shifted(value, axis, step):
    peers = lax.axis_size(axis)
    if peers == 1:
        return value
    return lax.ppermute(value, axis, [(i, (i + step) % peers) for i in range(peers)])


def extend(value, axis, dim, width):
    length = value.shape[dim]
    last = lax.slice_in_dim(value, length - width, length, axis=dim)
    first = lax.slice_in_dim(value, 0, width, axis=dim)
    return jnp.concatenate([shifted(last, axis, 1), value, shifted(first, axis, -1)], axis=dim)


def z_peers(value):
    below = shifted(value, "gz", 1)
    above = below if lax.axis_size("gz") <= 2 else shifted(value, "gz", -1)
    return below, above


def lane_iota(rows):
    return lax.broadcasted_iota(jnp.int32, (rows, lanes), 1)


def same_cell(group):
    row = lax.broadcasted_iota(jnp.int32, (lanes, lanes), 0)
    col = lax.broadcasted_iota(jnp.int32, (lanes, lanes), 1)
    return jnp.where(row // group == col // group, 1.0, 0.0).astype(jnp.float32)


def windows(own, below, above, group):
    lane = lane_iota(own.shape[0])
    down = jnp.where(lane < group, pltpu.roll(below, group, 1), pltpu.roll(own, group, 1))
    up = jnp.where(
        lane >= lanes - group,
        pltpu.roll(above, lanes - group, 1),
        pltpu.roll(own, lanes - group, 1),
    )
    return down, own, up


def pieces(value):
    parts = []
    for _ in range(3):
        part = value.astype(jnp.bfloat16)
        parts.append(part)
        value = value - part.astype(jnp.float32)
    return parts


def exact_dot(value, ones, contract):
    ones = ones.astype(jnp.bfloat16)
    total = None
    for part in pieces(value):
        left, right = (ones, part) if contract == 1 else (part, ones)
        term = lax.dot_general(
            left, right, (((1,), (contract,)), ((), ())), preferred_element_type=jnp.float32
        )
        total = term if total is None else total + term
    return total


def pick_mask(group):
    sub = lax.broadcasted_iota(jnp.int32, (group, lanes), 0)
    return (lane_iota(group) % group) == sub


def spread(rows, group, cell_sum):
    pick = pick_mask(group)
    total = None
    ones = cell_sum.astype(jnp.bfloat16)
    for part in pieces(rows):
        part = part.astype(jnp.float32)
        tall = jnp.concatenate(
            [jnp.where(pick, part[r : r + 1], 0.0) for r in range(rows.shape[0])], axis=0
        ).astype(jnp.bfloat16)
        term = jnp.dot(tall, ones, preferred_element_type=jnp.float32)
        total = term if total is None else total + term
    return total


def gather_rows(tall, group):
    pick = pick_mask(group)
    parts = tall.shape[0] // group
    return jnp.concatenate(
        [
            jnp.sum(jnp.where(pick, tall[p * group : (p + 1) * group], 0.0), axis=0, keepdims=True)
            for p in range(parts)
        ],
        axis=0,
    )


def placed(rows, x, y, parts):
    row = lax.broadcasted_iota(jnp.int32, rows.shape, 0)
    along_x = jnp.where(row < parts, unit, 0.0)
    along_y = jnp.where((row >= parts) & (row < 2 * parts), unit, 0.0)
    at_x, at_y = jnp.asarray(x).astype(jnp.float32), jnp.asarray(y).astype(jnp.float32)
    return rows + (along_x * at_x + along_y * at_y)


def fill_windows(own_ref, below_ref, above_ref, win_ref, square_ref, first, count_x, count_y,
                 parts, group):
    center_x = 0.5 * (count_x - 1)
    center_y = 0.5 * (count_y - 1)
    row = lax.broadcasted_iota(jnp.int32, (4 * parts, lanes), 0)
    z_step = jnp.where((row >= 2 * parts) & (row < 3 * parts), unit, 0.0)

    def step(x, carry):
        for y in range(count_y):
            tiles = windows(
                own_ref[x + first, y + first],
                below_ref[x + first, y + first],
                above_ref[x + first, y + first],
                group,
            )
            for k, tile in enumerate(tiles):
                tile = placed(tile, x - center_x, y - center_y, parts) + (k - 1.0) * z_step
                n = (x * count_y + y) * 3 + k
                win_ref[n] = tile
                if square_ref is not None:
                    square = tile * tile
                    square_ref[n] = -(
                        square[:parts] + square[parts : 2 * parts] + square[2 * parts : 3 * parts]
                    )
        return carry

    lax.fori_loop(0, count_x, step, 0)


def type_ratio(weight):
    return jnp.where(weight > 1.2, 1.4 / 1.6, jnp.where(weight > 0.0, 1.0, 0.0))


def density_kernel(own_ref, below_ref, above_ref, rows_ref, win_ref, square_ref, full_ref,
                   sum_ref, *, slots, group):
    wide_x, wide_y = own_ref.shape[0], own_ref.shape[1]
    parts = slots // group
    cell_sum = same_cell(group)
    fill_windows(own_ref, below_ref, above_ref, win_ref, square_ref, 0, wide_x, wide_y, parts,
                 group)
    inner_x, inner_y = wide_x - 2, wide_y - 2

    def spread_step(x, carry):
        for y in range(inner_y):
            rows = win_ref[((x + 1) * wide_y + y + 1) * 3 + 1]
            full_ref[x * inner_y + y] = spread(rows, group, cell_sum)
        return carry

    lax.fori_loop(0, inner_x, spread_step, 0)

    def column(n, carry):
        x, y = n // inner_y, n % inner_y
        px, py, pz = [full_ref[n, c * slots : (c + 1) * slots, :] for c in range(3)]
        room = reach - (px * px + py * py + pz * pz)
        px, py, pz = px + px, py + py, pz + pz

        total = jnp.zeros((slots, lanes), jnp.float32)
        for dx in range(3):
            base = ((x + dx) * wide_y + y) * 3
            for m in range(9):
                for p in range(parts):
                    jx, jy, jz, jw = [
                        win_ref[base + m, c * parts + p : c * parts + p + 1, :] for c in range(4)
                    ]
                    js = square_ref[base + m, p : p + 1, :]
                    margin = jnp.maximum((room + js) + px * jx + (py * jy + pz * jz), 0.0)
                    total = total + (jnp.exp2(margin) * margin) * (margin * jw)
        sum_ref[n] = total
        return carry

    lax.fori_loop(0, inner_x * inner_y, column, 0)

    def finish(x, carry):
        for y in range(inner_y):
            n = x * inner_y + y
            pw = full_ref[n, 3 * slots : 4 * slots, :]
            total = exact_dot(sum_ref[n], cell_sum, 0)
            density = jnp.maximum(total - self_density * pw, 0.0) * density_scale
            rows_ref[n] = gather_rows(jnp.sqrt(density + 1.0), group)
        return carry

    lax.fori_loop(0, inner_x, finish, 0)


def force_kernel(
    own_ref, below_ref, above_ref, rows_ref, rows_below_ref, rows_above_ref,
    out_ref, win_ref, slope_win_ref, full_ref, sum_ref, *, slots, group
):
    size_x, size_y, cells_z = out_ref.shape[0], out_ref.shape[1], out_ref.shape[2]
    wide_x, wide_y = size_x + 2, size_y + 2
    parts = slots // group
    cell_sum = same_cell(group)
    fill_windows(own_ref, below_ref, above_ref, win_ref, None, 1, wide_x, wide_y, parts, group)

    def slope_step(x, carry):
        for y in range(wide_y):
            n = x * wide_y + y
            tiles = windows(rows_ref[n], rows_below_ref[n], rows_above_ref[n], group)
            for k, tile in enumerate(tiles):
                weight = win_ref[n * 3 + k, 3 * parts : 4 * parts, :]
                slope_win_ref[n * 3 + k] = -type_ratio(weight) * (0.5 / decay) / tile
        return carry

    lax.fori_loop(0, wide_x, slope_step, 0)
    of_cell = jnp.where(
        lane_iota(cells_z) // group == lax.broadcasted_iota(jnp.int32, (cells_z, lanes), 0),
        1.0,
        0.0,
    ).astype(jnp.float32)

    def spread_step(x, carry):
        for y in range(size_y):
            rows = win_ref[((x + 1) * wide_y + y + 1) * 3 + 1]
            rows = jnp.concatenate([rows, rows_ref[(x + 1) * wide_y + y + 1]], axis=0)
            full_ref[x * size_y + y] = spread(rows, group, cell_sum)
        return carry

    lax.fori_loop(0, size_x, spread_step, 0)
    half = slots // 2

    def column(n, carry):
        x, y = n // size_y, n % size_y
        for start in (0, half):
            px, py, pz, pw, root = [
                full_ref[n, c * slots + start : c * slots + start + half, :] for c in range(5)
            ]
            pt = -type_ratio(pw) * (0.5 / decay) / root

            def side(dx, sums):
                fx, fy, fz, en = sums
                base = ((x + dx) * wide_y + y) * 3
                for m in range(9):
                    for p in range(parts):
                        jx, jy, jz, jw = [
                            win_ref[base + m, c * parts + p : c * parts + p + 1, :]
                            for c in range(4)
                        ]
                        jt = slope_win_ref[base + m, p : p + 1, :]
                        ax, ay, az = jx - px, jy - py, jz - pz
                        margin = jnp.maximum(reach - (ax * ax + ay * ay + az * az), 0.0)
                        power = jnp.exp2(margin)
                        edge = power * margin
                        weighted = edge * jw
                        v = weighted * (
                            (pt + jt) * (margin + slope_offset)
                            + power * (margin + 0.5 * slope_offset)
                        )
                        fx, fy, fz = fx + v * ax, fy + v * ay, fz + v * az
                        en = en + weighted * edge
                return fx, fy, fz, en

            zero = jnp.zeros((half, lanes), jnp.float32)
            fx, fy, fz, en = lax.fori_loop(0, 3, side, (zero, zero, zero, zero))
            embedding = jnp.where(pw > 1.2, 1.4, pw)
            scale = force_scale * pw
            sum_ref[n, start : start + half, :] = fx * scale
            sum_ref[n, slots + start : slots + start + half, :] = fy * scale
            sum_ref[n, 2 * slots + start : 2 * slots + start + half, :] = fz * scale
            sum_ref[n, 3 * slots + start : 3 * slots + start + half, :] = (
                en - (self_energy / group) * pw
            ) * (energy_scale * pw) - embedding * root * (1.0 / group)
        return carry

    lax.fori_loop(0, size_x * size_y, column, 0)

    def finish(x, carry):
        for y in range(size_y):
            out_ref[x, y] = exact_dot(sum_ref[x * size_y + y], of_cell, 1)
        return carry

    lax.fori_loop(0, size_x, finish, 0)


def in_vmem(*values):
    kept = [pltpu.with_memory_space_constraint(value, pltpu.VMEM) for value in values]
    return kept, [pl.BlockSpec(memory_space=pltpu.VMEM) for _ in values]


def body(positions, types):
    size_x, size_y, cells_z, slots = types.shape
    group = lanes // cells_z
    parts = slots // group
    weight = jnp.where(types == 1, 1.0, jnp.where(types == 2, 1.6, 0.0)).astype(jnp.float32)
    value = jnp.concatenate([positions * unit, weight], axis=3)
    value = value.reshape(size_x, size_y, cells_z, 4 * parts, group)
    value = value.transpose(0, 1, 3, 2, 4).reshape(size_x, size_y, 4 * parts, lanes)
    value = extend(extend(value, "gx", 0, 2), "gy", 1, 2)
    below, above = z_peers(value)
    columns = (size_x + 2) * (size_y + 2)
    f32 = jnp.float32
    operands, specs = in_vmem(value, below, above)
    root_rows = pl.pallas_call(
        lambda *refs: density_kernel(*refs, slots=slots, group=group),
        out_shape=pltpu.VMEM((columns, parts, lanes), f32),
        in_specs=specs,
        out_specs=pl.BlockSpec(memory_space=pltpu.VMEM),
        scratch_shapes=[
            pltpu.VMEM(((size_x + 4) * (size_y + 4) * 3, 4 * parts, lanes), f32),
            pltpu.VMEM(((size_x + 4) * (size_y + 4) * 3, parts, lanes), f32),
            pltpu.VMEM((columns, 4 * slots, lanes), f32),
            pltpu.VMEM((columns, slots, lanes), f32),
        ],
        name="density",
    )(*operands)
    root_below, root_above = z_peers(root_rows)
    operands, specs = in_vmem(value, below, above, root_rows, root_below, root_above)
    return pl.pallas_call(
        lambda *refs: force_kernel(*refs, slots=slots, group=group),
        out_shape=jax.ShapeDtypeStruct((size_x, size_y, cells_z, 4 * slots), f32),
        in_specs=specs,
        scratch_shapes=[
            pltpu.VMEM((columns * 3, 4 * parts, lanes), f32),
            pltpu.VMEM((columns * 3, parts, lanes), f32),
            pltpu.VMEM((size_x * size_y, 5 * slots, lanes), f32),
            pltpu.VMEM((size_x * size_y, 4 * slots, lanes), f32),
        ],
        name="force",
    )(*operands)


def solution(mesh):
    in_specs = (P("gx", "gy", "gz", None), P("gx", "gy", "gz", None))
    out_specs = P("gx", "gy", "gz", None)
    return jax.shard_map(body, mesh=mesh, in_specs=in_specs, out_specs=out_specs, check_vma=False)
```
